128 devices in a mesh: node: 8 (over x, core), dev: 16 (over y, z).
Axes of the slice: x: 4, y: 4, z: 4, core: 2. Of those that a mesh axis runs over, the one named last changes fastest.
Arguments:
- expert_hidden: bfloat16 [131072, 1536], P(('node', 'dev')), may hold values from -6 to 6
- expert_down: bfloat16 [128, 1536, 5120], P(('node', 'dev')), may hold values from -0.15625 to 0.15625
- shared_hidden: bfloat16 [16384, 1536], P(('node', 'dev')), may hold values from -6 to 6
- shared_down: bfloat16 [1536, 5120], P('dev'), may hold values from -0.15625 to 0.15625
- expert_ids: int32 [16384, 6], P(('node', 'dev')), may hold values from 0 to 127, as said below
- gates: float32 [16384, 6], P(('node', 'dev')), may hold values from 0.1 to 2
Outputs:
- combined: bfloat16 [16384, 5120], P(('node', 'dev'))
The draws below stay inside these ranges and needn't reach their ends.
Inputs may be any that keep to these rules, and one draw needn't show every extreme that they name: `expert_ids`: each row names 6 different experts, two in each of three different groups, expert e lying in group e // 16. Among the 128 rows of one device every group is named by exactly 48 rows and no expert by more than 8 rows; some expert is named by exactly 8 rows of every device.
All inputs are finite; a program needn't handle non-finite values.
Results may differ from the reference program's by a relative error of at most 0.0047.
Values may be sent and summed in bfloat16 or wider, within the bound.
A program may use at most 128 MiB of HBM per device.

```python
import math
import jax
import jax.numpy as jnp
from jax import lax

D = 5120
EF = 1536
SH = 1536
TOP = 6
TOK_DEV = 128
NODES = 8
NODE_EXP = 16
EXPERTS = 128
CAP = 8
SLOTS = 1024
TOKENS = 16384


def one_block(block_key, full_expert):
    order_key, score_key, shift_key, token_key, column_key = jax.random.split(block_key, 5)
    half_cap = CAP // 2
    label_count = NODE_EXP * half_cap
    node_share = 3 * TOK_DEV // NODES
    node_order = jax.random.permutation(order_key, NODES).astype(jnp.int32)
    scores = jax.random.randint(score_key, (NODES, label_count), 0, 65536)
    label_expert = jnp.arange(label_count, dtype=jnp.int32) % NODE_EXP
    shifts = jax.random.randint(shift_key, (NODES,), 1, NODE_EXP)
    full_node = full_expert // NODE_EXP
    full_local = full_expert % NODE_EXP
    partner = (full_local - shifts) % NODE_EXP
    forced = (node_order[:, None] == full_node) & ((label_expert[None, :] == full_local) | (label_expert[None, :] == partner[:, None]))
    ranked = (scores - forced.astype(jnp.int32) * 131072) * label_count + jnp.arange(label_count, dtype=jnp.int32)[None, :]
    sequence = jnp.argsort(ranked, axis=1)
    first_expert = (sequence % NODE_EXP)[:, :node_share]
    second_expert = (first_expert + shifts[:, None]) % NODE_EXP
    places = jnp.arange(TOK_DEV, dtype=jnp.int32)[:, None] * 3 + jnp.arange(3, dtype=jnp.int32)[None, :]
    node_place = places % NODES
    node_rank = places // NODES
    chosen_node = node_order[node_place]
    first_pick = chosen_node * NODE_EXP + first_expert[node_place, node_rank]
    second_pick = chosen_node * NODE_EXP + second_expert[node_place, node_rank]
    picked = jnp.stack([first_pick, second_pick], axis=2).reshape(TOK_DEV, TOP)
    picked = picked[jax.random.permutation(token_key, TOK_DEV)]
    column_scores = jax.random.randint(column_key, (TOK_DEV, TOP), 0, 65536) * TOP + jnp.arange(TOP, dtype=jnp.int32)[None, :]
    column_order = jnp.argsort(column_scores, axis=1)
    return jnp.take_along_axis(picked, column_order, axis=1).astype(jnp.int32)


def draw_expert_ids(key, part):
    full_expert = jax.random.randint(jax.random.fold_in(key, 7), (), 0, EXPERTS)
    block_keys = jax.random.split(jax.random.fold_in(key, 11), TOKENS // TOK_DEV)
    picked = jax.vmap(lambda block_key: one_block(block_key, full_expert))(block_keys)
    return picked.reshape(TOKENS, TOP)


def level_of(rng, shape, pieces, smallest, largest):
    def one(dim, parts):
        draws = jax.random.uniform(jax.random.fold_in(jax.random.fold_in(rng, 6), dim), (parts,), jnp.float32, smallest / len(pieces), largest / len(pieces))
        return jnp.repeat(jnp.exp(draws), shape[dim] // parts).reshape((-1,) + (1,) * (len(shape) - dim - 1))

    factor_of = one(*pieces[0])
    for cut in pieces[1:]:
        factor_of = factor_of * one(*cut)
    return factor_of


def normal_values(own_key, shape, width, reach, pieces=(), held_as=jnp.bfloat16):
    result = jax.random.normal(own_key, shape, jnp.float32) * width
    if len(pieces) > 0:
        result = level_of(own_key, shape, pieces, -0.22, 0.18) * result
    return jnp.clip(result, min=-reach, max=reach).astype(held_as)


def setup_inputs(seed: int = 0) -> dict:
    key_list = jax.random.split(jax.random.key(seed), 7)
    return {
        "expert_hidden": normal_values(key_list[0], (EXPERTS * SLOTS, EF), 1.0, 6.0, ((0, 128),)),
        "expert_down": normal_values(key_list[1], (EXPERTS, EF, D), EF ** -0.5, 0.15625, ((0, 128),)),
        "shared_hidden": normal_values(key_list[2], (TOKENS, SH), 1.0, 6.0, ((0, 128),)),
        "shared_down": normal_values(key_list[3], (SH, D), SH ** -0.5, 0.15625, ((0, 16),)),
        "expert_ids": draw_expert_ids(jax.random.fold_in(key_list[6], 71), 0),
        "gates": jnp.clip(jnp.exp(math.log(2.0) - 2.9957323 * jax.random.uniform(key_list[5], (TOKENS, TOP), jnp.float32) ** level_of(key_list[5], (TOKENS, TOP), ((0, 128),), -0.2, 0.2)), 0.1, 2.0),
    }


def reference(expert_hidden, expert_down, shared_hidden, shared_down, expert_ids, gates):
    blocks = expert_ids.reshape(EXPERTS, TOK_DEV, TOP)
    labels = jnp.arange(EXPERTS, dtype=jnp.int32)
    chosen = (blocks[..., None] == labels).astype(jnp.int32)
    counts = jnp.sum(chosen, axis=2)
    before = jnp.cumsum(counts, axis=1) - counts
    position = jnp.sum(chosen * before[:, :, None, :], axis=3).astype(jnp.int32)
    source = jnp.arange(EXPERTS, dtype=jnp.int32)[:, None, None]
    slot_index = (blocks * SLOTS + source * CAP + position).reshape(-1).astype(jnp.int32)
    owner_rows = jnp.repeat(jnp.arange(TOKENS, dtype=jnp.int32), TOP)
    slot_owner = jnp.zeros((EXPERTS * SLOTS,), jnp.int32).at[slot_index].set(owner_rows)
    slot_gate = jnp.zeros((EXPERTS * SLOTS,), jnp.float32).at[slot_index].set(gates.reshape(-1).astype(jnp.float32))
    hidden_blocks = expert_hidden.reshape(EXPERTS, SLOTS, EF)

    def one_expert(running, inputs):
        hidden, weight, owners, weights = inputs
        product = jnp.dot(hidden.astype(jnp.float32), weight.astype(jnp.float32), preferred_element_type=jnp.float32)
        rounded = lax.optimization_barrier(product.astype(jnp.bfloat16)).astype(jnp.float32)
        return running.at[owners].add(weights[:, None] * rounded), None

    routed, unused = lax.scan(one_expert, jnp.zeros((TOKENS, D), jnp.float32),
                              (hidden_blocks, expert_down, slot_owner.reshape(EXPERTS, SLOTS), slot_gate.reshape(EXPERTS, SLOTS)))
    shared = jnp.dot(shared_hidden, shared_down, preferred_element_type=jnp.float32)
    return (shared + routed).astype(jnp.bfloat16)
```

```python
import functools

import jax
import jax.numpy as jnp
from jax import lax
from jax.experimental import pallas as pl
from jax.experimental.pallas import tpu as pltpu
from jax.sharding import PartitionSpec as P

MESH = pl.DeviceIdType.MESH
BF = jnp.bfloat16
F32 = jnp.float32
NODES = 8
RING = 4
CAP = 8
EXPERTS = 128
TOK = 128
TOP = 6
EF = 1536
D = 5120
KS = 384
C = 256
HALF = D // 2
STEPS = HALF // C
SLOTS = 3
NODE_OFFSETS = ((1, 0), (3, 0), (2, 0), (1, 1), (3, 1), (2, 1), (0, 1))


def iota(shape, dim):
    return lax.broadcasted_iota(jnp.int32, shape, dim)


def dot(a, b):
    return jnp.dot(a, b, preferred_element_type=F32)


def kernel(
    hid_h, wd_h, sh_h, shz_h, sd_h, ids_ref, gates_ref, out_h,
    hid, wbuf, obuf, recv1, recv2, recv3, pbuf, wg, gbig, hrecv, grecv, gsend, outv,
    load_sem, w_sem, own_sem, init_send, init_recv, send1, rsem1, send2, rsem2, send3, rsem3, out_sem,
):
    n = lax.axis_index("node")
    d = lax.axis_index("dev")
    x, core = n // 2, n % 2
    y, z = d // RING, d % RING

    def node_at(offset):
        ox, oc = offset
        return ((x + ox) % RING) * 2 + (core + oc) % 2

    def along(kind, step):
        if kind == 0:
            to = (z + step) % RING
            return to, y * RING + to
        to = (y + step) % RING
        return to, to * RING + z

    mine = (z, y)

    def load_w(step, slot):
        for k in range(2):
            col = pl.multiple_of(k * HALF + step * C, C)
            yield pltpu.make_async_copy(wd_h.at[:, pl.ds(col, C)], wbuf.at[slot, k], w_sem.at[slot, k])

    hid_copy = pltpu.make_async_copy(hid_h, hid, load_sem)
    hid_copy.start()
    for copy in load_w(0, 0):
        copy.start()
    own_copies = (
        pltpu.make_async_copy(sd_h.at[:, pl.ds(0, HALF)], wg.at[0, z], own_sem.at[0]),
        pltpu.make_async_copy(sd_h.at[:, pl.ds(HALF, HALF)], wg.at[1, y], own_sem.at[1]),
        pltpu.make_async_copy(sh_h.at[:, pl.ds(pl.multiple_of(y * KS, KS), KS)], hrecv.at[0, y], own_sem.at[2]),
        pltpu.make_async_copy(shz_h.at[z], hrecv.at[1, z], own_sem.at[3]),
    )
    for copy in own_copies:
        copy.start()

    barrier = pltpu.get_barrier_semaphore()
    for offset in NODE_OFFSETS:
        pl.semaphore_signal(barrier, inc=1, device_id=(node_at(offset), d), device_id_type=MESH)
    for kind in range(2):
        for step in range(1, RING):
            pl.semaphore_signal(barrier, inc=1, device_id=(n, along(kind, step)[1]), device_id_type=MESH)
    pl.semaphore_wait(barrier, len(NODE_OFFSETS) + 2 * (RING - 1))

    def remote(src, dst, ssem, rsem, node, dev):
        pltpu.make_async_remote_copy(
            src_ref=src, dst_ref=dst, send_sem=ssem, recv_sem=rsem, device_id=(node, dev), device_id_type=MESH
        ).start()

    def take(ref, sem):
        pltpu.make_async_copy(ref, ref, sem).wait()

    for step in (1, 3, 2):
        to, dev = along(1, step)
        remote(sh_h.at[:, pl.ds(pl.multiple_of(to * KS, KS), KS)], hrecv.at[0, y], init_send.at[0], init_recv.at[0], n, dev)
        to, dev = along(0, step)
        remote(shz_h.at[to], hrecv.at[1, z], init_send.at[1], init_recv.at[1], n, dev)
    for step in (1, 3, 2):
        _, dev = along(0, step)
        remote(sd_h.at[:, pl.ds(0, HALF)], wg.at[0, z], init_send.at[2], init_recv.at[2], n, dev)
        _, dev = along(1, step)
        remote(sd_h.at[:, pl.ds(HALF, HALF)], wg.at[1, y], init_send.at[3], init_recv.at[3], n, dev)

    def gate_pieces():
        label = iota((EXPERTS, TOK), 0)
        chosen = jnp.zeros((EXPERTS, TOK), F32)
        weight = jnp.zeros((EXPERTS, TOK), F32)
        for k in range(TOP):
            hit = ids_ref[k:k + 1, :] == label
            chosen += jnp.where(hit, 1.0, 0.0)
            weight += jnp.where(hit, gates_ref[k:k + 1, :], 0.0)
        earlier = (iota((TOK, TOK), 0) < iota((TOK, TOK), 1)).astype(F32).astype(BF)
        place = dot(chosen.astype(BF), earlier)
        place = jnp.where(chosen > 0.5, place, 255.0)
        place = jnp.transpose(place).astype(BF)
        weight = jnp.transpose(weight).astype(BF)
        lanes = CAP * EXPERTS // RING
        row = iota((EXPERTS, lanes), 0)
        lane = iota((EXPERTS, lanes), 1)
        other, group = lane // (CAP * NODES), (lane // CAP) % NODES
        slot = (iota((TOK, lanes), 1) % CAP).astype(F32)
        for k in range(2):
            for target in range(RING):
                local = target * RING + other if k == 0 else other * RING + target
                spread = jnp.where(row == group * (RING * RING) + local, 1.0, 0.0).astype(BF)
                piece = jnp.where(dot(place, spread) == slot, dot(weight, spread), 0.0)
                gsend[k, target] = piece.astype(BF)
        for k in range(2):
            own = mine[1 - k]
            grecv[k, own] = gsend[k, own]
            for step in (1, 3, 2):
                to, dev = along(1 - k, step)
                remote(gsend.at[k, to], grecv.at[k, own], init_send.at[4 + k], init_recv.at[4 + k], n, dev)

    def widen_gates():
        for k in range(2):
            take(grecv.at[k, pl.ds(0, RING - 1)], init_recv.at[4 + k])
        lanes = CAP * EXPERTS // RING
        row = iota((lanes, RING * lanes), 0)
        lane = iota((lanes, RING * lanes), 1)
        same = (row // CAP == lane // (RING * CAP)) & (row % CAP == lane % CAP)
        part = (lane // CAP) % RING
        for target in range(RING):
            spread = jnp.where(same & (part == target), 1.0, 0.0).astype(BF)
            for k in range(2):
                gbig[k, pl.ds(target * TOK, TOK), :] = dot(grecv[k, target], spread).astype(BF)
        for k in range(2):
            take(hrecv.at[k, pl.ds(0, RING - 1)], init_recv.at[k])
            take(wg.at[k, pl.ds(0, RING - 1)], init_recv.at[2 + k])
        for copy in own_copies:
            copy.wait()

    hid_copy.wait()

    def multiply(step):
        slot = step % 2
        place = step % SLOTS
        for copy in load_w(step, slot):
            copy.wait()

        @pl.when(step + 1 < STEPS)
        def _():
            for copy in load_w(step + 1, (step + 1) % 2):
                copy.start()

        @pl.when(step >= SLOTS)
        def _():
            for k in range(2):
                take(obuf.at[place, k, pl.ds(0, NODES - 1)], send1.at[place, k])

        for k in range(2):
            for part in range(2):
                rows = part * 512
                o = dot(hid[rows:rows + 512, :], wbuf[slot, k])
                if k == 0:
                    o = jnp.concatenate(
                        [
                            o[b * 128 + yy * 32 + zz * 8:b * 128 + yy * 32 + zz * 8 + 8]
                            for b in range(4) for zz in range(RING) for yy in range(RING)
                        ],
                        axis=0,
                    )
                obuf[place, k, pl.ds(part * 4, 4)] = o.astype(BF).reshape(4, 128, C)
            for offset in NODE_OFFSETS:
                to = node_at(offset)
                remote(obuf.at[place, k, to], recv1.at[k, step, n], send1.at[place, k], rsem1.at[k, step], to, d)
            recv1[k, step, n] = obuf[place, k, n]

    def forward(step):
        for k in range(2):
            take(recv1.at[k, step, pl.ds(0, NODES - 1)], rsem1.at[k, step])
            for hop in (1, 3, 2):
                to, dev = along(k, hop)
                rows = pl.multiple_of(to * 32, 32)
                remote(recv1.at[k, step, :, pl.ds(rows, 32), :], recv2.at[k, step, mine[k]], send2.at[k, step], rsem2.at[k, step], n, dev)
            rows = pl.multiple_of(mine[k] * 32, 32)
            recv2[k, step, mine[k]] = recv1[k, step, :, pl.ds(rows, 32), :]

    def combine(step):
        for k in range(2):
            take(recv2.at[k, step, pl.ds(0, RING - 1)], rsem2.at[k, step])
            slots = recv2[k, step].reshape(1024, C)
            cols = pl.multiple_of(step * C, C)
            weights = wg[k, :, :, pl.ds(cols, C)].reshape(KS, C)
            part = dot(gbig[k], slots) + dot(hrecv[k].reshape(RING * TOK, KS), weights)
            pbuf[k, step] = part.astype(BF).reshape(RING, TOK, C)
            own = mine[1 - k]
            for hop in (1, 3, 2):
                to, dev = along(1 - k, hop)
                remote(pbuf.at[k, step, to], recv3.at[k, step, own], send3.at[k, step], rsem3.at[k, step], n, dev)
            recv3[k, step, own] = pbuf[k, step, own]

    def out_copy(k, step):
        col = pl.multiple_of(k * HALF + step * C, C)
        return pltpu.make_async_copy(outv.at[k, step], out_h.at[:, pl.ds(col, C)], out_sem.at[k, step])

    def finish(step):
        for k in range(2):
            take(recv3.at[k, step, pl.ds(0, RING - 1)], rsem3.at[k, step])
            total = recv3[k, step, 0].astype(F32)
            for j in range(1, RING):
                total += recv3[k, step, j].astype(F32)
            outv[k, step] = total.astype(BF)
            out_copy(k, step).start()

    def loop(i, carry):
        @pl.when(i < STEPS)
        def _():
            multiply(i)

        @pl.when(i == 0)
        def _():
            gate_pieces()

        @pl.when((i >= 1) & (i < STEPS + 1))
        def _():
            forward(i - 1)

        @pl.when(i == 1)
        def _():
            widen_gates()

        @pl.when((i >= 2) & (i < STEPS + 2))
        def _():
            combine(i - 2)

        @pl.when(i >= 3)
        def _():
            finish(i - 3)

        return carry

    lax.fori_loop(0, STEPS + 3, loop, 0)

    for k in range(2):
        take(hrecv.at[k, pl.ds(0, RING - 1)], init_send.at[k])
        take(wg.at[k, pl.ds(0, RING - 1)], init_send.at[2 + k])
        take(gsend.at[k, pl.ds(0, RING - 1)], init_send.at[4 + k])
        for place in range(SLOTS):
            take(obuf.at[place, k, pl.ds(0, NODES - 1)], send1.at[place, k])

    def drain(step, carry):
        for k in range(2):
            take(recv2.at[k, step, pl.ds(0, RING - 1)], send2.at[k, step])
            take(recv3.at[k, step, pl.ds(0, RING - 1)], send3.at[k, step])
            out_copy(k, step).wait()
        return carry

    lax.fori_loop(0, STEPS, drain, 0)


def body(expert_hidden, expert_down, shared_hidden, shared_down, expert_ids, gates):
    hidden_z = shared_hidden.reshape(TOK, RING, RING, 96).transpose(2, 0, 1, 3).reshape(RING, TOK, KS)
    anywhere = pl.BlockSpec(memory_space=pl.ANY)
    vmem = pl.BlockSpec(memory_space=pltpu.VMEM)
    dma = pltpu.SemaphoreType.DMA
    return pl.pallas_call(
        kernel,
        out_shape=jax.ShapeDtypeStruct((TOK, D), BF),
        in_specs=[anywhere] * 5 + [vmem] * 2,
        out_specs=anywhere,
        scratch_shapes=[
            pltpu.VMEM((1024, EF), BF),
            pltpu.VMEM((2, 2, EF, C), BF),
            pltpu.VMEM((SLOTS, 2, NODES, 128, C), BF),
            pltpu.VMEM((2, STEPS, NODES, 128, C), BF),
            pltpu.VMEM((2, STEPS, RING, NODES, 32, C), BF),
            pltpu.VMEM((2, STEPS, RING, TOK, C), BF),
            pltpu.VMEM((2, STEPS, RING, TOK, C), BF),
            pltpu.VMEM((2, RING, 96, HALF), BF),
            pltpu.VMEM((2, RING * TOK, 1024), BF),
            pltpu.VMEM((2, RING, TOK, KS), BF),
            pltpu.VMEM((2, RING, TOK, 256), BF),
            pltpu.VMEM((2, RING, TOK, 256), BF),
            pltpu.VMEM((2, STEPS, TOK, C), BF),
            dma,
            dma((2, 2)),
            dma((4,)),
            dma((6,)),
            dma((6,)),
            dma((SLOTS, 2)),
            dma((2, STEPS)),
            dma((2, STEPS)),
            dma((2, STEPS)),
            dma((2, STEPS)),
            dma((2, STEPS)),
            dma((2, STEPS)),
        ],
        compiler_params=pltpu.CompilerParams(
            collective_id=0, has_side_effects=True, vmem_limit_bytes=64 * 1024 * 1024 - 65536
        ),
        name="combine",
    )(
        expert_hidden,
        expert_down.reshape(EF, D),
        shared_hidden,
        hidden_z,
        shared_down,
        expert_ids.T,
        gates.T,
    )


def solution(mesh):
    in_specs = (
        P(("node", "dev"), None),
        P(("node", "dev"), None, None),
        P(("node", "dev"), None),
        P("dev", None),
        P(("node", "dev"), None),
        P(("node", "dev"), None),
    )
    out_specs = P(("node", "dev"), None)
    return jax.shard_map(body, mesh=mesh, in_specs=in_specs, out_specs=out_specs, check_vma=False)
```

```python
import functools

import jax
import jax.numpy as jnp
from jax import lax
from jax.experimental import pallas as pl
from jax.experimental.pallas import tpu as pltpu
from jax.sharding import PartitionSpec as P

MESH = pl.DeviceIdType.MESH
BF = jnp.bfloat16
F32 = jnp.float32
NODES = 8
RING = 4
CAP = 8
EXPERTS = 128
TOK = 128
TOP = 6
EF = 1536
D = 5120
KS = 384
C = 128
WIDE = 256
PARTS = WIDE // C
HALF = D // 2
STEPS = HALF // C
ROUNDS = HALF // WIDE
AHEAD = 2
SLOTS = AHEAD + 2
NODE_OFFSETS = ((1, 0), (3, 0), (2, 0), (1, 1), (3, 1), (2, 1), (0, 1))


def iota(shape, dim):
    return lax.broadcasted_iota(jnp.int32, shape, dim)


def dot(a, b):
    return jnp.dot(a, b, preferred_element_type=F32)


def kernel(
    hid_h, wd_h, sh_h, sd_h, ids_h, gates_h, out_ref,
    hid, sh_ref, ids_ref, gates_ref, wbuf, obuf, recv1, recv2, recv3, pbuf, wg, gbig, hrecv, grecv, hsend, gsend,
    load_sem, w_sem, own_sem, init_send, init_recv, send1, rsem1, send2, rsem2, send3, rsem3,
):
    n = lax.axis_index("node")
    d = lax.axis_index("dev")
    x, core = n // 2, n % 2
    y, z = d // RING, d % RING

    def node_at(offset):
        ox, oc = offset
        return ((x + ox) % RING) * 2 + (core + oc) % 2

    def along(kind, step):
        if kind == 0:
            to = (z + step) % RING
            return to, y * RING + to
        to = (y + step) % RING
        return to, to * RING + z

    mine = (z, y)

    def load_w(step, slot):
        for k in range(2):
            col = pl.multiple_of(k * HALF + step * WIDE, WIDE)
            yield pltpu.make_async_copy(wd_h.at[:, pl.ds(col, WIDE)], wbuf.at[slot, k], w_sem.at[slot, k])

    hid_copy = pltpu.make_async_copy(hid_h, hid, load_sem)
    hid_copy.start()
    for copy in load_w(0, 0):
        copy.start()
    small_copies = (
        pltpu.make_async_copy(sh_h, sh_ref, own_sem.at[2]),
        pltpu.make_async_copy(ids_h, ids_ref, own_sem.at[3]),
        pltpu.make_async_copy(gates_h, gates_ref, own_sem.at[4]),
    )
    own_copies = (
        pltpu.make_async_copy(sd_h.at[:, pl.ds(0, HALF)], wg.at[0, z], own_sem.at[0]),
        pltpu.make_async_copy(sd_h.at[:, pl.ds(HALF, HALF)], wg.at[1, y], own_sem.at[1]),
    )
    for copy in small_copies + own_copies:
        copy.start()

    barrier = pltpu.get_barrier_semaphore()
    for offset in NODE_OFFSETS:
        pl.semaphore_signal(barrier, inc=1, device_id=(node_at(offset), d), device_id_type=MESH)
    for kind in range(2):
        for step in range(1, RING):
            pl.semaphore_signal(barrier, inc=1, device_id=(n, along(kind, step)[1]), device_id_type=MESH)
    pl.semaphore_wait(barrier, len(NODE_OFFSETS) + 2 * (RING - 1))

    def remote(src, dst, ssem, rsem, node, dev):
        pltpu.make_async_remote_copy(
            src_ref=src, dst_ref=dst, send_sem=ssem, recv_sem=rsem, device_id=(node, dev), device_id_type=MESH
        ).start()

    def take(ref, sem):
        pltpu.make_async_copy(ref, ref, sem).wait()

    def set_up():
        for step in (1, 3, 2):
            _, dev = along(0, step)
            remote(sd_h.at[:, pl.ds(0, HALF)], wg.at[0, z], init_send.at[2], init_recv.at[2], n, dev)
            _, dev = along(1, step)
            remote(sd_h.at[:, pl.ds(HALF, HALF)], wg.at[1, y], init_send.at[3], init_recv.at[3], n, dev)
        for copy in small_copies:
            copy.wait()
        for target in range(RING):
            hsend[0, target] = sh_ref[:, target * KS:(target + 1) * KS]
            hsend[1, target] = jnp.concatenate(
                [sh_ref[:, (other * RING + target) * 96:(other * RING + target + 1) * 96] for other in range(RING)], axis=1
            )
        for k in range(2):
            own = mine[1 - k]
            hrecv[k, own] = hsend[k, own]
            for step in (1, 3, 2):
                to, dev = along(1 - k, step)
                remote(hsend.at[k, to], hrecv.at[k, own], init_send.at[k], init_recv.at[k], n, dev)

    def gate_pieces():
        label = iota((EXPERTS, TOK), 0)
        chosen = jnp.zeros((EXPERTS, TOK), F32)
        weight = jnp.zeros((EXPERTS, TOK), F32)
        for k in range(TOP):
            hit = ids_ref[k:k + 1, :] == label
            chosen += jnp.where(hit, 1.0, 0.0)
            weight += jnp.where(hit, gates_ref[k:k + 1, :], 0.0)
        earlier = (iota((TOK, TOK), 0) < iota((TOK, TOK), 1)).astype(F32).astype(BF)
        place = dot(chosen.astype(BF), earlier)
        place = jnp.where(chosen > 0.5, place, 255.0)
        place = jnp.transpose(place).astype(BF)
        weight = jnp.transpose(weight).astype(BF)
        lanes = CAP * EXPERTS // RING
        row = iota((EXPERTS, lanes), 0)
        lane = iota((EXPERTS, lanes), 1)
        other, group = lane // (CAP * NODES), (lane // CAP) % NODES
        slot = (iota((TOK, lanes), 1) % CAP).astype(F32)
        for k in range(2):
            for target in range(RING):
                local = target * RING + other if k == 0 else other * RING + target
                spread = jnp.where(row == group * (RING * RING) + local, 1.0, 0.0).astype(BF)
                piece = jnp.where(dot(place, spread) == slot, dot(weight, spread), 0.0)
                gsend[k, target] = piece.astype(BF)
        for k in range(2):
            own = mine[1 - k]
            grecv[k, own] = gsend[k, own]
            for step in (1, 3, 2):
                to, dev = along(1 - k, step)
                remote(gsend.at[k, to], grecv.at[k, own], init_send.at[4 + k], init_recv.at[4 + k], n, dev)

    def widen_gates():
        for k in range(2):
            take(grecv.at[k, pl.ds(0, RING - 1)], init_recv.at[4 + k])
        lanes = CAP * EXPERTS // RING
        row = iota((lanes, RING * lanes), 0)
        lane = iota((lanes, RING * lanes), 1)
        same = (row // CAP == lane // (RING * CAP)) & (row % CAP == lane % CAP)
        part = (lane // CAP) % RING
        for target in range(RING):
            spread = jnp.where(same & (part == target), 1.0, 0.0).astype(BF)
            for k in range(2):
                gbig[k, pl.ds(target * TOK, TOK), :] = dot(grecv[k, target], spread).astype(BF)
        for k in range(2):
            take(hrecv.at[k, pl.ds(0, RING - 1)], init_recv.at[k])
            take(wg.at[k, pl.ds(0, RING - 1)], init_recv.at[2 + k])
        for copy in own_copies:
            copy.wait()

    hid_copy.wait()

    def multiply(step):
        slot = step % 2
        place = step % SLOTS
        for copy in load_w(step, slot):
            copy.wait()

        @pl.when(step + 1 < ROUNDS)
        def _():
            for copy in load_w(step + 1, (step + 1) % 2):
                copy.start()

        @pl.when(step >= SLOTS)
        def _():
            for k in range(2):
                for h in range(PARTS):
                    take(obuf.at[place, k, h, pl.ds(0, NODES - 1)], send1.at[place, k, h])

        for k in range(2):
            for part in range(2):
                rows = part * 512
                o = dot(hid[rows:rows + 512, :], wbuf[slot, k])
                if k == 0:
                    o = jnp.concatenate(
                        [
                            o[b * 128 + yy * 32 + zz * 8:b * 128 + yy * 32 + zz * 8 + 8]
                            for b in range(4) for zz in range(RING) for yy in range(RING)
                        ],
                        axis=0,
                    )
                o = o.astype(BF)
                for h in range(PARTS):
                    obuf[place, k, h, pl.ds(part * 4, 4)] = o[:, h * C:(h + 1) * C].reshape(4, 128, C)
            for h in range(PARTS):
                small = step * PARTS + h
                for offset in NODE_OFFSETS:
                    to = node_at(offset)
                    remote(obuf.at[place, k, h, to], recv1.at[k, small, n], send1.at[place, k, h], rsem1.at[k, small], to, d)
                recv1[k, small, n] = obuf[place, k, h, n]

    def forward(k, step):
        take(recv1.at[k, step, pl.ds(0, NODES - 1)], rsem1.at[k, step])
        for hop in (1, 3, 2):
            to, dev = along(k, hop)
            rows = pl.multiple_of(to * 32, 32)
            remote(recv1.at[k, step, :, pl.ds(rows, 32), :], recv2.at[k, step, mine[k]], send2.at[k, step], rsem2.at[k, step], n, dev)
        rows = pl.multiple_of(mine[k] * 32, 32)
        recv2[k, step, mine[k]] = recv1[k, step, :, pl.ds(rows, 32), :]

    def combine(k, step):
        take(recv2.at[k, step, pl.ds(0, RING - 1)], rsem2.at[k, step])
        slots = recv2[k, step].reshape(1024, C)
        cols = pl.multiple_of(step * C, C)
        weights = wg[k, :, :, pl.ds(cols, C)].reshape(KS, C)
        part = dot(gbig[k], slots) + dot(hrecv[k].reshape(RING * TOK, KS), weights)
        pbuf[k, step] = part.astype(BF).reshape(RING, TOK, C)
        own = mine[1 - k]
        for hop in (1, 3, 2):
            to, dev = along(1 - k, hop)
            remote(pbuf.at[k, step, to], recv3.at[k, step, own], send3.at[k, step], rsem3.at[k, step], n, dev)
        recv3[k, step, own] = pbuf[k, step, own]

    def finish(k, step):
        take(recv3.at[k, step, pl.ds(0, RING - 1)], rsem3.at[k, step])
        total = recv3[k, step, 0].astype(F32)
        for j in range(1, RING):
            total += recv3[k, step, j].astype(F32)
        out_ref[:, pl.ds(pl.multiple_of(k * HALF + step * C, C), C)] = total.astype(BF)

    def stage(i, lag, act):
        @pl.when((i >= lag) & (i < ROUNDS + lag))
        def _():
            for k in range(2):
                for h in range(PARTS):
                    act(k, (i - lag) * PARTS + h)

    def loop(i, carry):
        @pl.when(i < ROUNDS)
        def _():
            multiply(i)

        @pl.when(i == 0)
        def _():
            set_up()
            gate_pieces()

        stage(i, AHEAD, forward)

        @pl.when(i == AHEAD + 1)
        def _():
            widen_gates()

        stage(i, AHEAD + 1, combine)
        stage(i, AHEAD + 2, finish)
        return carry

    lax.fori_loop(0, ROUNDS + AHEAD + 2, loop, 0)

    for k in range(2):
        take(hsend.at[k, pl.ds(0, RING - 1)], init_send.at[k])
        take(wg.at[k, pl.ds(0, RING - 1)], init_send.at[2 + k])
        take(gsend.at[k, pl.ds(0, RING - 1)], init_send.at[4 + k])
        for h in range(PARTS):
            for place in range(SLOTS):
                take(obuf.at[place, k, h, pl.ds(0, NODES - 1)], send1.at[place, k, h])

    def drain(step, carry):
        for k in range(2):
            take(recv2.at[k, step, pl.ds(0, RING - 1)], send2.at[k, step])
            take(recv3.at[k, step, pl.ds(0, RING - 1)], send3.at[k, step])
        return carry

    lax.fori_loop(0, STEPS, drain, 0)


def body(expert_hidden, expert_down, shared_hidden, shared_down, expert_ids, gates):
    anywhere = pl.BlockSpec(memory_space=pl.ANY)
    vmem = pl.BlockSpec(memory_space=pltpu.VMEM)
    dma = pltpu.SemaphoreType.DMA
    return pl.pallas_call(
        kernel,
        out_shape=pltpu.VMEM((TOK, D), BF),
        in_specs=[anywhere] * 6,
        out_specs=vmem,
        scratch_shapes=[
            pltpu.VMEM((1024, EF), BF),
            pltpu.VMEM((TOK, EF), BF),
            pltpu.VMEM((TOP, TOK), jnp.int32),
            pltpu.VMEM((TOP, TOK), F32),
            pltpu.VMEM((2, 2, EF, WIDE), BF),
            pltpu.VMEM((SLOTS, 2, PARTS, NODES, 128, C), BF),
            pltpu.VMEM((2, STEPS, NODES, 128, C), BF),
            pltpu.VMEM((2, STEPS, RING, NODES, 32, C), BF),
            pltpu.VMEM((2, STEPS, RING, TOK, C), BF),
            pltpu.VMEM((2, STEPS, RING, TOK, C), BF),
            pltpu.VMEM((2, RING, 96, HALF), BF),
            pltpu.VMEM((2, RING * TOK, 1024), BF),
            pltpu.VMEM((2, RING, TOK, KS), BF),
            pltpu.VMEM((2, RING, TOK, 256), BF),
            pltpu.VMEM((2, RING, TOK, KS), BF),
            pltpu.VMEM((2, RING, TOK, 256), BF),
            dma,
            dma((2, 2)),
            dma((5,)),
            dma((6,)),
            dma((6,)),
            dma((SLOTS, 2, PARTS)),
            dma((2, STEPS)),
            dma((2, STEPS)),
            dma((2, STEPS)),
            dma((2, STEPS)),
            dma((2, STEPS)),
        ],
        compiler_params=pltpu.CompilerParams(
            collective_id=0, has_side_effects=True, vmem_limit_bytes=56 * 1024 * 1024
        ),
        name="combine",
    )(
        expert_hidden,
        expert_down.reshape(EF, D),
        shared_hidden,
        shared_down,
        expert_ids.T,
        gates.T,
    )


def solution(mesh):
    in_specs = (
        P(("node", "dev"), None),
        P(("node", "dev"), None, None),
        P(("node", "dev"), None),
        P("dev", None),
        P(("node", "dev"), None),
        P(("node", "dev"), None),
    )
    out_specs = P(("node", "dev"), None)
    return jax.shard_map(body, mesh=mesh, in_specs=in_specs, out_specs=out_specs, check_vma=False)
```

```python
import functools

import jax
import jax.numpy as jnp
from jax import lax
from jax.experimental import pallas as pl
from jax.experimental.pallas import tpu as pltpu
from jax.sharding import PartitionSpec as P

MESH = pl.DeviceIdType.MESH
BF = jnp.bfloat16
F32 = jnp.float32
NODES = 8
RING = 4
CAP = 8
EXPERTS = 128
TOK = 128
TOP = 6
EF = 1536
D = 5120
KS = 384
C = 128
WIDE = 256
PARTS = WIDE // C
HALF = D // 2
XR = 2
ROUNDS = HALF // WIDE - XR
ALL = ROUNDS + XR
LAST = ROUNDS - 1
PACK = 48
QUART = HALF // 2
AHEAD = 3
SLOTS = AHEAD + 2
NODE_OFFSETS = ((1, 0), (3, 0), (2, 0), (1, 1), (3, 1), (2, 1), (0, 1))


def iota(shape, dim):
    return lax.broadcasted_iota(jnp.int32, shape, dim)


def dot(a, b):
    return jnp.dot(a, b, preferred_element_type=F32)


def kernel(
    hid_h, wd_h, sh_h, sd_h, ids_h, gates_h, out_ref,
    hid, sh_ref, ids_ref, gates_ref, wbuf, obuf, recv1, recv2, recv3, pbuf, wg, gbig, hrecv, grecv, hsend, gsend,
    xbuf, xr1, xr2, xr3, xpart, abig, asend, arecv, place_back,
    load_sem, w_sem, own_sem, init_send, init_recv, send1, rsem1, send2, rsem2, send3, rsem3,
    xs1, xq1, xs2, xq2, xs3, xq3, ash, arc,
):
    n = lax.axis_index("node")
    d = lax.axis_index("dev")
    x, core = n // 2, n % 2
    y, z = d // RING, d % RING

    def node_at(offset):
        ox, oc = offset
        return ((x + ox) % RING) * 2 + (core + oc) % 2

    def along(kind, step):
        if kind == 0:
            to = (z + step) % RING
            return to, y * RING + to
        to = (y + step) % RING
        return to, to * RING + z

    mine = (z, y)

    def my_quart(base):
        return pl.ds(pl.multiple_of(base + core * QUART, 128), QUART)

    def load_w(step, slot):
        for k in range(2):
            col = pl.multiple_of(k * HALF + step * WIDE, WIDE)
            yield pltpu.make_async_copy(wd_h.at[:, pl.ds(col, WIDE)], wbuf.at[slot, k], w_sem.at[slot, k])

    hid_copy = pltpu.make_async_copy(hid_h, hid, load_sem)
    hid_copy.start()
    for copy in load_w(0, 0):
        copy.start()
    small_copies = (
        pltpu.make_async_copy(sh_h, sh_ref, own_sem.at[2]),
        pltpu.make_async_copy(ids_h, ids_ref, own_sem.at[3]),
        pltpu.make_async_copy(gates_h, gates_ref, own_sem.at[4]),
    )
    own_copies = (
        pltpu.make_async_copy(sd_h.at[:, my_quart(0)], wg.at[0, z, :, my_quart(0)], own_sem.at[0]),
        pltpu.make_async_copy(sd_h.at[:, my_quart(HALF)], wg.at[1, y, :, my_quart(0)], own_sem.at[1]),
    )
    for copy in small_copies + own_copies:
        copy.start()

    barrier = pltpu.get_barrier_semaphore()
    for offset in NODE_OFFSETS:
        pl.semaphore_signal(barrier, inc=1, device_id=(node_at(offset), d), device_id_type=MESH)
    for kind in range(2):
        for step in range(1, RING):
            pl.semaphore_signal(barrier, inc=1, device_id=(n, along(kind, step)[1]), device_id_type=MESH)
    pl.semaphore_wait(barrier, len(NODE_OFFSETS) + 2 * (RING - 1))

    def remote(src, dst, ssem, rsem, node, dev):
        pltpu.make_async_remote_copy(
            src_ref=src, dst_ref=dst, send_sem=ssem, recv_sem=rsem, device_id=(node, dev), device_id_type=MESH
        ).start()

    def take(ref, sem):
        pltpu.make_async_copy(ref, ref, sem).wait()

    def send_rows():
        for step in (1, 3, 2):
            _, dev = along(0, step)
            remote(sd_h.at[:, my_quart(0)], wg.at[0, z, :, my_quart(0)], init_send.at[2], init_recv.at[2], n, dev)
            _, dev = along(1, step)
            remote(sd_h.at[:, my_quart(HALF)], wg.at[1, y, :, my_quart(0)], init_send.at[3], init_recv.at[3], n, dev)

    def set_up():
        for copy in small_copies:
            copy.wait()
        for target in range(RING):
            hsend[0, target] = sh_ref[:, target * KS:(target + 1) * KS]
            hsend[1, target] = jnp.concatenate(
                [sh_ref[:, (other * RING + target) * 96:(other * RING + target + 1) * 96] for other in range(RING)], axis=1
            )
        for k in range(2):
            own = mine[1 - k]
            hrecv[k, own] = hsend[k, own]
            for step in (1, 3, 2):
                to, dev = along(1 - k, step)
                remote(hsend.at[k, to], hrecv.at[k, own], init_send.at[k], init_recv.at[k], n, dev)

    def gate_pieces():
        label = iota((EXPERTS, TOK), 0)
        chosen = jnp.zeros((EXPERTS, TOK), F32)
        weight = jnp.zeros((EXPERTS, TOK), F32)
        for k in range(TOP):
            hit = ids_ref[k:k + 1, :] == label
            chosen += jnp.where(hit, 1.0, 0.0)
            weight += jnp.where(hit, gates_ref[k:k + 1, :], 0.0)
        earlier = (iota((TOK, TOK), 0) < iota((TOK, TOK), 1)).astype(F32).astype(BF)
        place = dot(chosen.astype(BF), earlier)
        place = jnp.where(chosen > 0.5, place, 255.0)
        named = jnp.sum(chosen.reshape(NODES, EXPERTS // NODES, TOK), axis=1) * 0.5
        rank = dot(named.astype(BF), earlier)
        rank = jnp.where(named > 0.5, rank, 255.0)
        pick = jnp.concatenate(
            [jnp.where(iota((PACK, TOK), 0).astype(F32) == rank[g:g + 1, :], 1.0, 0.0) for g in range(NODES)], axis=0
        )
        place_back[...] = jnp.transpose(pick).astype(BF)
        pick = pick.astype(BF)
        place = jnp.transpose(place).astype(BF)
        weight = jnp.transpose(weight).astype(BF)
        lanes = CAP * EXPERTS // RING
        row = iota((EXPERTS, lanes), 0)
        lane = iota((EXPERTS, lanes), 1)
        other, group = lane // (CAP * NODES), (lane // CAP) % NODES
        slot = (iota((TOK, lanes), 1) % CAP).astype(F32)
        for k in range(2):
            for target in range(RING):
                local = target * RING + other if k == 0 else other * RING + target
                spread = jnp.where(row == group * (RING * RING) + local, 1.0, 0.0).astype(BF)
                piece = jnp.where(dot(place, spread) == slot, dot(weight, spread), 0.0)
                gsend[k, target] = piece.astype(BF)
        row = iota((EXPERTS, EXPERTS), 0)
        lane = iota((EXPERTS, EXPERTS), 1)
        slot = (iota((TOK, EXPERTS), 1) % CAP).astype(F32)
        for g in range(NODES):
            spread = jnp.where(row == g * (RING * RING) + lane // CAP, 1.0, 0.0).astype(BF)
            piece = jnp.where(dot(place, spread) == slot, dot(weight, spread), 0.0).astype(BF)
            asend[g] = dot(pick[g * PACK:(g + 1) * PACK], piece).astype(BF)
        arecv[n] = asend[n]
        for offset in NODE_OFFSETS:
            to = node_at(offset)
            remote(asend.at[to], arecv.at[n], ash, arc, to, d)
        for k in range(2):
            own = mine[1 - k]
            grecv[k, own] = gsend[k, own]
            for step in (1, 3, 2):
                to, dev = along(1 - k, step)
                remote(gsend.at[k, to], grecv.at[k, own], init_send.at[4 + k], init_recv.at[4 + k], n, dev)

    def widen_gates():
        for k in range(2):
            take(grecv.at[k, pl.ds(0, RING - 1)], init_recv.at[4 + k])
        lanes = CAP * EXPERTS // RING
        row = iota((lanes, RING * lanes), 0)
        lane = iota((lanes, RING * lanes), 1)
        same = (row // CAP == lane // (RING * CAP)) & (row % CAP == lane % CAP)
        part = (lane // CAP) % RING
        for target in range(RING):
            spread = jnp.where(same & (part == target), 1.0, 0.0).astype(BF)
            for k in range(2):
                gbig[k, pl.ds(target * TOK, TOK), :] = dot(grecv[k, target], spread).astype(BF)
        for k in range(2):
            take(hrecv.at[k, pl.ds(0, RING - 1)], init_recv.at[k])
            take(wg.at[k, :, :, pl.ds(0, QUART)], init_recv.at[6 + k])

    def share_rows():
        for copy in own_copies:
            copy.wait()
        for k in range(2):
            take(wg.at[k, pl.ds(0, RING - 1), :, pl.ds(0, QUART)], init_recv.at[2 + k])
            half = wg.at[k, :, :, my_quart(0)]
            remote(half, half, init_send.at[6 + k], init_recv.at[6 + k], x * 2 + 1 - core, d)

    def widen_x():
        take(arecv.at[pl.ds(0, NODES - 1)], arc)
        row = iota((EXPERTS, 1024), 0)
        lane = iota((EXPERTS, 1024), 1)
        outer, inner, node = lane // 256, (lane // 64) % RING, (lane // CAP) % NODES
        for k in range(2):
            local = outer * RING + inner if k == 0 else inner * RING + outer
            same = (row // CAP == local) & (row % CAP == lane % CAP)
            for m in range(NODES):
                spread = jnp.where(same & (node == m), 1.0, 0.0).astype(BF)
                abig[k, m * PACK:(m + 1) * PACK, :] = dot(arecv[m], spread).astype(BF)

    def x_multiply(xr):
        for copy in load_w(ROUNDS + xr, xr):
            copy.wait()
        for copy in load_w(ROUNDS + 1 if xr == 0 else 2, 1 - xr):
            copy.start()
        for k in range(2):
            for part in range(2):
                rows = part * 512
                o = dot(hid[rows:rows + 512, :], wbuf[xr, k])
                pieces = []
                for outer in range(RING):
                    for inner in range(RING):
                        yy, zz = (inner, outer) if k == 0 else (outer, inner)
                        for b in range(4):
                            at = b * 128 + yy * 32 + zz * 8
                            pieces.append(o[at:at + 8])
                o = jnp.concatenate(pieces, axis=0).astype(BF)
                xbuf[k, xr, :, :, part * 32:(part + 1) * 32, :] = o.reshape(RING, RING, 32, WIDE)
            for hop in (1, 3, 2):
                to, dev = along(k, hop)
                remote(xbuf.at[k, xr, to], xr1.at[k, xr, mine[k]], xs1.at[k, xr], xq1.at[k, xr], n, dev)
            xr1[k, xr, mine[k]] = xbuf[k, xr, mine[k]]

    def x_forward(xr):
        for k in range(2):
            take(xr1.at[k, xr, pl.ds(0, RING - 1)], xq1.at[k, xr])
            own = mine[1 - k]
            for hop in (1, 3, 2):
                to, dev = along(1 - k, hop)
                remote(xr1.at[k, xr, :, to], xr2.at[k, xr, own], xs2.at[k, xr], xq2.at[k, xr], n, dev)
            xr2[k, xr, own] = xr1[k, xr, :, own]

    def x_combine(xr):
        for k in range(2):
            take(xr2.at[k, xr, pl.ds(0, RING - 1)], xq2.at[k, xr])
            part = dot(abig[k], xr2[k, xr].reshape(1024, WIDE))
            xpart[k, xr] = part.astype(BF).reshape(NODES, PACK, WIDE)
            for offset in NODE_OFFSETS:
                to = node_at(offset)
                remote(xpart.at[k, xr, to], xr3.at[k, xr, n], xs3.at[k, xr], xq3.at[k, xr], to, d)
            xr3[k, xr, n] = xpart[k, xr, n]
            weights = wg[k, :, :, (ROUNDS + xr) * WIDE:(ROUNDS + xr + 1) * WIDE].reshape(KS, WIDE)
            send_part(k, ROUNDS + xr, 0, WIDE, ROUNDS + 1 + xr, dot(hrecv[k].reshape(RING * TOK, KS), weights))

    def x_finish(xr):
        for k in range(2):
            take(xr3.at[k, xr, pl.ds(0, NODES - 1)], xq3.at[k, xr])
            routed = dot(place_back[...], xr3[k, xr].reshape(NODES * PACK, WIDE))
            finish(k, ROUNDS + xr, 0, WIDE, ROUNDS + 1 + xr, routed)


    def multiply(step):
        first = isinstance(step, int)
        slot = step % 2
        place = step % SLOTS
        for copy in load_w(step, slot):
            copy.wait()
        if first:
            for copy in load_w(1 if step == 0 else ROUNDS, 1 - slot):
                copy.start()
        else:
            @pl.when(step + 1 < ROUNDS)
            def _():
                for copy in load_w(step + 1, (step + 1) % 2):
                    copy.start()

            @pl.when(step >= SLOTS)
            def _():
                for k in range(2):
                    take(obuf.at[place, k, pl.ds(0, NODES - 1)], send1.at[place, k, 0])

        def send(k, lane, width, h):
            cols = pl.ds(lane, width)
            for offset in NODE_OFFSETS:
                to = node_at(offset)
                remote(
                    obuf.at[place, k, to, :, cols], recv1.at[k, step, n, :, cols],
                    send1.at[place, k, h], rsem1.at[k, step + h], to, d,
                )

        for k in range(2):
            for part in range(2):
                rows = part * 512
                o = dot(hid[rows:rows + 512, :], wbuf[slot, k])
                if k == 0:
                    o = jnp.concatenate(
                        [
                            o[b * 128 + yy * 32 + zz * 8:b * 128 + yy * 32 + zz * 8 + 8]
                            for b in range(4) for zz in range(RING) for yy in range(RING)
                        ],
                        axis=0,
                    )
                obuf[place, k, pl.ds(part * 4, 4)] = o.astype(BF).reshape(4, 128, WIDE)
            if first:
                send(k, 0, WIDE, 0)
            else:
                @pl.when(step < LAST)
                def _():
                    send(k, 0, WIDE, 0)

                @pl.when(step == LAST)
                def _():
                    for h in range(PARTS):
                        send(k, h * C, C, h)
            recv1[k, step, n] = obuf[place, k, n]

    def forward(k, step, lane, width, sem):
        cols = pl.ds(lane, width)
        take(recv1.at[k, step, pl.ds(0, NODES - 1), :, cols], rsem1.at[k, sem])
        for hop in (1, 3, 2):
            to, dev = along(k, hop)
            rows = pl.multiple_of(to * 32, 32)
            remote(
                recv1.at[k, step, :, pl.ds(rows, 32), cols], recv2.at[k, step, mine[k], :, :, cols],
                send2.at[k, sem], rsem2.at[k, sem], n, dev,
            )
        rows = pl.multiple_of(mine[k] * 32, 32)
        recv2[k, step, mine[k], :, :, cols] = recv1[k, step, :, pl.ds(rows, 32), cols]

    def combine(k, step, lane, width, sem):
        cols = pl.ds(lane, width)
        take(recv2.at[k, step, pl.ds(0, RING - 1), :, :, cols], rsem2.at[k, sem])
        slots = recv2[k, step, :, :, :, cols].reshape(1024, width)
        wide = pl.ds(pl.multiple_of(step * WIDE + lane, 128), width)
        weights = wg[k, :, :, wide].reshape(KS, width)
        send_part(k, step, lane, width, sem, dot(gbig[k], slots) + dot(hrecv[k].reshape(RING * TOK, KS), weights))

    def send_part(k, step, lane, width, sem, part):
        cols = pl.ds(lane, width)
        pbuf[k, step, :, :, cols] = part.astype(BF).reshape(RING, TOK, width)
        own = mine[1 - k]
        for hop in (1, 3, 2):
            to, dev = along(1 - k, hop)
            remote(
                pbuf.at[k, step, to, :, cols], recv3.at[k, step, own, :, cols],
                send3.at[k, sem], rsem3.at[k, sem], n, dev,
            )
        recv3[k, step, own, :, cols] = pbuf[k, step, own, :, cols]

    def finish(k, step, lane, width, sem, extra=None):
        cols = pl.ds(lane, width)
        take(recv3.at[k, step, pl.ds(0, RING - 1), :, cols], rsem3.at[k, sem])
        total = recv3[k, step, 0, :, cols].astype(F32)
        for j in range(1, RING):
            total += recv3[k, step, j, :, cols].astype(F32)
        if extra is not None:
            total += extra
        out_ref[:, pl.ds(pl.multiple_of(k * HALF + step * WIDE + lane, 128), width)] = total.astype(BF)

    def stage(i, lag, act):
        @pl.when((i >= lag) & (i < LAST + lag))
        def _():
            for k in range(2):
                act(k, i - lag, 0, WIDE, i - lag)

        @pl.when(i == LAST + lag)
        def _():
            for k in range(2):
                for h in range(PARTS):
                    act(k, LAST, h * C, C, LAST + h)

    def loop(i, carry):
        @pl.when(i < ROUNDS)
        def _():
            multiply(i)

        stage(i, AHEAD, forward)

        @pl.when((i == 2) | (i == 3))
        def _():
            x_forward(i - 2)

        pl.when(i == AHEAD)(share_rows)
        pl.when(i == AHEAD + 1)(widen_gates)
        stage(i, AHEAD + 1, combine)
        pl.when(i == AHEAD + 2)(widen_x)

        for xr in range(XR):
            @pl.when(i == AHEAD + 3 + xr)
            def _():
                x_combine(xr)

            @pl.when(i == AHEAD + 5 + xr)
            def _():
                x_finish(xr)

        stage(i, AHEAD + 2, finish)
        return carry

    send_rows()
    hid_copy.wait()
    multiply(0)
    multiply(1)
    for xr in range(XR):
        x_multiply(xr)
    set_up()
    gate_pieces()
    lax.fori_loop(2, ROUNDS + AHEAD + 2, loop, 0)

    for k in range(2):
        take(hsend.at[k, pl.ds(0, RING - 1)], init_send.at[k])
        take(wg.at[k, pl.ds(0, RING - 1), :, pl.ds(0, QUART)], init_send.at[2 + k])
        take(wg.at[k, :, :, pl.ds(0, QUART)], init_send.at[6 + k])
        take(gsend.at[k, pl.ds(0, RING - 1)], init_send.at[4 + k])
        for xr in range(XR):
            take(xbuf.at[k, xr, pl.ds(0, RING - 1)], xs1.at[k, xr])
            take(xr2.at[k, xr, pl.ds(0, RING - 1)], xs2.at[k, xr])
            take(xpart.at[k, xr, pl.ds(0, NODES - 1)], xs3.at[k, xr])
        for step in range(ROUNDS - SLOTS, LAST):
            take(obuf.at[step % SLOTS, k, pl.ds(0, NODES - 1)], send1.at[step % SLOTS, k, 0])
        for h in range(PARTS):
            cols = pl.ds(h * C, C)
            take(obuf.at[LAST % SLOTS, k, pl.ds(0, NODES - 1), :, cols], send1.at[LAST % SLOTS, k, h])
            take(recv2.at[k, LAST, pl.ds(0, RING - 1), :, :, cols], send2.at[k, LAST + h])
            take(recv3.at[k, LAST, pl.ds(0, RING - 1), :, cols], send3.at[k, LAST + h])
        for xr in range(XR):
            take(recv3.at[k, ROUNDS + xr, pl.ds(0, RING - 1)], send3.at[k, ROUNDS + 1 + xr])
    take(asend.at[pl.ds(0, NODES - 1)], ash)

    def drain(step, carry):
        for k in range(2):
            take(recv2.at[k, step, pl.ds(0, RING - 1)], send2.at[k, step])
            take(recv3.at[k, step, pl.ds(0, RING - 1)], send3.at[k, step])
        return carry

    lax.fori_loop(0, LAST, drain, 0)


def body(expert_hidden, expert_down, shared_hidden, shared_down, expert_ids, gates):
    anywhere = pl.BlockSpec(memory_space=pl.ANY)
    vmem = pl.BlockSpec(memory_space=pltpu.VMEM)
    dma = pltpu.SemaphoreType.DMA
    return pl.pallas_call(
        kernel,
        out_shape=pltpu.VMEM((TOK, D), BF),
        in_specs=[anywhere] * 6,
        out_specs=vmem,
        scratch_shapes=[
            pltpu.VMEM((1024, EF), BF),
            pltpu.VMEM((TOK, EF), BF),
            pltpu.VMEM((TOP, TOK), jnp.int32),
            pltpu.VMEM((TOP, TOK), F32),
            pltpu.VMEM((2, 2, EF, WIDE), BF),
            pltpu.VMEM((SLOTS, 2, NODES, 128, WIDE), BF),
            pltpu.VMEM((2, ROUNDS, NODES, 128, WIDE), BF),
            pltpu.VMEM((2, ROUNDS, RING, NODES, 32, WIDE), BF),
            pltpu.VMEM((2, ALL, RING, TOK, WIDE), BF),
            pltpu.VMEM((2, ALL, RING, TOK, WIDE), BF),
            pltpu.VMEM((2, RING, 96, HALF), BF),
            pltpu.VMEM((2, RING * TOK, 1024), BF),
            pltpu.VMEM((2, RING, TOK, KS), BF),
            pltpu.VMEM((2, RING, TOK, 256), BF),
            pltpu.VMEM((2, RING, TOK, KS), BF),
            pltpu.VMEM((2, RING, TOK, 256), BF),
            pltpu.VMEM((2, XR, RING, RING, 64, WIDE), BF),
            pltpu.VMEM((2, XR, RING, RING, 64, WIDE), BF),
            pltpu.VMEM((2, XR, RING, RING, 64, WIDE), BF),
            pltpu.VMEM((2, XR, NODES, PACK, WIDE), BF),
            pltpu.VMEM((2, XR, NODES, PACK, WIDE), BF),
            pltpu.VMEM((2, NODES * PACK, 1024), BF),
            pltpu.VMEM((NODES, PACK, EXPERTS), BF),
            pltpu.VMEM((NODES, PACK, EXPERTS), BF),
            pltpu.VMEM((TOK, NODES * PACK), BF),
            dma,
            dma((2, 2)),
            dma((5,)),
            dma((8,)),
            dma((8,)),
            dma((SLOTS, 2, PARTS)),
            dma((2, ALL + 1)),
            dma((2, ALL + 1)),
            dma((2, ALL + 1)),
            dma((2, ALL + 1)),
            dma((2, ALL + 1)),
            dma((2, XR)),
            dma((2, XR)),
            dma((2, XR)),
            dma((2, XR)),
            dma((2, XR)),
            dma((2, XR)),
            dma,
            dma,
        ],
        compiler_params=pltpu.CompilerParams(
            collective_id=0, has_side_effects=True, vmem_limit_bytes=60 * 1024 * 1024
        ),
        name="combine",
    )(
        expert_hidden,
        expert_down.reshape(EF, D),
        shared_hidden,
        shared_down,
        expert_ids.T,
        gates.T,
    )


def solution(mesh):
    in_specs = (
        P(("node", "dev"), None),
        P(("node", "dev"), None, None),
        P(("node", "dev"), None),
        P("dev", None),
        P(("node", "dev"), None),
        P(("node", "dev"), None),
    )
    out_specs = P(("node", "dev"), None)
    return jax.shard_map(body, mesh=mesh, in_specs=in_specs, out_specs=out_specs, check_vma=False)
```

```python
import functools

import jax
import jax.numpy as jnp
from jax import lax
from jax.experimental import pallas as pl
from jax.experimental.pallas import tpu as pltpu
from jax.sharding import PartitionSpec as P

MESH = pl.DeviceIdType.MESH
BF = jnp.bfloat16
F32 = jnp.float32
NODES = 8
RING = 4
CAP = 8
EXPERTS = 128
TOK = 128
TOP = 6
EF = 1536
D = 5120
KS = 384
C = 128
WIDE = 256
PARTS = WIDE // C
HALF = D // 2
XR = 2
ROUNDS = HALF // WIDE - XR
ALL = ROUNDS + XR
LAST = ROUNDS - 1
PACK = 48
QUART = HALF // 2
AHEAD = 3
SLOTS = AHEAD + 2
NODE_OFFSETS = ((2, 0), (2, 1), (1, 0), (3, 0), (1, 1), (3, 1), (0, 1))


def iota(shape, dim):
    return lax.broadcasted_iota(jnp.int32, shape, dim)


def dot(a, b):
    return jnp.dot(a, b, preferred_element_type=F32)


def kernel(
    hid_h, wd_h, sh_h, sd_h, ids_h, gates_h, out_ref,
    hid, sh_ref, ids_ref, gates_ref, wbuf, obuf, recv1, recv2, recv3, pbuf, wg, gbig, hrecv, grecv, hsend, gsend,
    xbuf, xr1, xr2, xr3, xpart, abig, asend, arecv, place_back,
    load_sem, w_sem, own_sem, init_send, init_recv, send1, rsem1, send2, rsem2, send3, rsem3,
    xs1, xq1, xs2, xq2, xs3, xq3, ash, arc,
):
    n = lax.axis_index("node")
    d = lax.axis_index("dev")
    x, core = n // 2, n % 2
    y, z = d // RING, d % RING

    def node_at(offset):
        ox, oc = offset
        return ((x + ox) % RING) * 2 + (core + oc) % 2

    def along(kind, step):
        if kind == 0:
            to = (z + step) % RING
            return to, y * RING + to
        to = (y + step) % RING
        return to, to * RING + z

    mine = (z, y)

    def my_quart(base):
        return pl.ds(pl.multiple_of(base + core * QUART, 128), QUART)

    def load_w(step, slot):
        for k in range(2):
            col = pl.multiple_of(k * HALF + step * WIDE, WIDE)
            yield pltpu.make_async_copy(wd_h.at[:, pl.ds(col, WIDE)], wbuf.at[slot, k], w_sem.at[slot, k])

    hid_copy = pltpu.make_async_copy(hid_h, hid, load_sem)
    hid_copy.start()
    for copy in load_w(0, 0):
        copy.start()
    small_copies = (
        pltpu.make_async_copy(sh_h, sh_ref, own_sem.at[2]),
        pltpu.make_async_copy(ids_h, ids_ref, own_sem.at[3]),
        pltpu.make_async_copy(gates_h, gates_ref, own_sem.at[4]),
    )
    own_copies = (
        pltpu.make_async_copy(sd_h.at[:, my_quart(0)], wg.at[0, z, :, my_quart(0)], own_sem.at[0]),
        pltpu.make_async_copy(sd_h.at[:, my_quart(HALF)], wg.at[1, y, :, my_quart(0)], own_sem.at[1]),
    )
    for copy in small_copies + own_copies:
        copy.start()

    barrier = pltpu.get_barrier_semaphore()
    for offset in NODE_OFFSETS:
        pl.semaphore_signal(barrier, inc=1, device_id=(node_at(offset), d), device_id_type=MESH)
    for kind in range(2):
        for step in range(1, RING):
            pl.semaphore_signal(barrier, inc=1, device_id=(n, along(kind, step)[1]), device_id_type=MESH)
    pl.semaphore_wait(barrier, len(NODE_OFFSETS) + 2 * (RING - 1))

    def remote(src, dst, ssem, rsem, node, dev):
        pltpu.make_async_remote_copy(
            src_ref=src, dst_ref=dst, send_sem=ssem, recv_sem=rsem, device_id=(node, dev), device_id_type=MESH
        ).start()

    def take(ref, sem):
        pltpu.make_async_copy(ref, ref, sem).wait()

    def send_rows():
        for step in (2, 1, 3):
            _, dev = along(0, step)
            remote(sd_h.at[:, my_quart(0)], wg.at[0, z, :, my_quart(0)], init_send.at[2], init_recv.at[2], n, dev)
            _, dev = along(1, step)
            remote(sd_h.at[:, my_quart(HALF)], wg.at[1, y, :, my_quart(0)], init_send.at[3], init_recv.at[3], n, dev)

    def set_up():
        for copy in small_copies:
            copy.wait()
        for target in range(RING):
            hsend[0, target] = sh_ref[:, target * KS:(target + 1) * KS]
            hsend[1, target] = jnp.concatenate(
                [sh_ref[:, (other * RING + target) * 96:(other * RING + target + 1) * 96] for other in range(RING)], axis=1
            )
        for k in range(2):
            own = mine[1 - k]
            hrecv[k, own] = hsend[k, own]
            for step in (2, 1, 3):
                to, dev = along(1 - k, step)
                remote(hsend.at[k, to], hrecv.at[k, own], init_send.at[k], init_recv.at[k], n, dev)

    def gate_pieces():
        label = iota((EXPERTS, TOK), 0)
        chosen = jnp.zeros((EXPERTS, TOK), F32)
        weight = jnp.zeros((EXPERTS, TOK), F32)
        for k in range(TOP):
            hit = ids_ref[k:k + 1, :] == label
            chosen += jnp.where(hit, 1.0, 0.0)
            weight += jnp.where(hit, gates_ref[k:k + 1, :], 0.0)
        earlier = (iota((TOK, TOK), 0) < iota((TOK, TOK), 1)).astype(F32).astype(BF)
        place = dot(chosen.astype(BF), earlier)
        place = jnp.where(chosen > 0.5, place, 255.0)
        named = jnp.sum(chosen.reshape(NODES, EXPERTS // NODES, TOK), axis=1) * 0.5
        rank = dot(named.astype(BF), earlier)
        rank = jnp.where(named > 0.5, rank, 255.0)
        pick = jnp.concatenate(
            [jnp.where(iota((PACK, TOK), 0).astype(F32) == rank[g:g + 1, :], 1.0, 0.0) for g in range(NODES)], axis=0
        )
        place_back[...] = jnp.transpose(pick).astype(BF)
        pick = pick.astype(BF)
        place = jnp.transpose(place).astype(BF)
        weight = jnp.transpose(weight).astype(BF)
        lanes = CAP * EXPERTS // RING
        row = iota((EXPERTS, lanes), 0)
        lane = iota((EXPERTS, lanes), 1)
        other, group = lane // (CAP * NODES), (lane // CAP) % NODES
        slot = (iota((TOK, lanes), 1) % CAP).astype(F32)
        for k in range(2):
            for target in range(RING):
                local = target * RING + other if k == 0 else other * RING + target
                spread = jnp.where(row == group * (RING * RING) + local, 1.0, 0.0).astype(BF)
                piece = jnp.where(dot(place, spread) == slot, dot(weight, spread), 0.0)
                gsend[k, target] = piece.astype(BF)
        row = iota((EXPERTS, EXPERTS), 0)
        lane = iota((EXPERTS, EXPERTS), 1)
        slot = (iota((TOK, EXPERTS), 1) % CAP).astype(F32)
        for g in range(NODES):
            spread = jnp.where(row == g * (RING * RING) + lane // CAP, 1.0, 0.0).astype(BF)
            piece = jnp.where(dot(place, spread) == slot, dot(weight, spread), 0.0).astype(BF)
            asend[g] = dot(pick[g * PACK:(g + 1) * PACK], piece).astype(BF)
        arecv[n] = asend[n]
        for offset in NODE_OFFSETS:
            to = node_at(offset)
            remote(asend.at[to], arecv.at[n], ash, arc, to, d)
        for k in range(2):
            own = mine[1 - k]
            grecv[k, own] = gsend[k, own]
            for step in (2, 1, 3):
                to, dev = along(1 - k, step)
                remote(gsend.at[k, to], grecv.at[k, own], init_send.at[4 + k], init_recv.at[4 + k], n, dev)

    def widen_gates():
        for k in range(2):
            take(grecv.at[k, pl.ds(0, RING - 1)], init_recv.at[4 + k])
        lanes = CAP * EXPERTS // RING
        row = iota((lanes, RING * lanes), 0)
        lane = iota((lanes, RING * lanes), 1)
        same = (row // CAP == lane // (RING * CAP)) & (row % CAP == lane % CAP)
        part = (lane // CAP) % RING
        for target in range(RING):
            spread = jnp.where(same & (part == target), 1.0, 0.0).astype(BF)
            for k in range(2):
                gbig[k, pl.ds(target * TOK, TOK), :] = dot(grecv[k, target], spread).astype(BF)
        for k in range(2):
            take(hrecv.at[k, pl.ds(0, RING - 1)], init_recv.at[k])
            take(wg.at[k, :, :, pl.ds(0, QUART)], init_recv.at[6 + k])

    def share_rows():
        for copy in own_copies:
            copy.wait()
        for k in range(2):
            take(wg.at[k, pl.ds(0, RING - 1), :, pl.ds(0, QUART)], init_recv.at[2 + k])
            half = wg.at[k, :, :, my_quart(0)]
            remote(half, half, init_send.at[6 + k], init_recv.at[6 + k], x * 2 + 1 - core, d)

    def widen_x():
        take(arecv.at[pl.ds(0, NODES - 1)], arc)
        row = iota((EXPERTS, 1024), 0)
        lane = iota((EXPERTS, 1024), 1)
        outer, inner, node = lane // 256, (lane // 64) % RING, (lane // CAP) % NODES
        for k in range(2):
            local = outer * RING + inner if k == 0 else inner * RING + outer
            same = (row // CAP == local) & (row % CAP == lane % CAP)
            for m in range(NODES):
                spread = jnp.where(same & (node == m), 1.0, 0.0).astype(BF)
                abig[k, m * PACK:(m + 1) * PACK, :] = dot(arecv[m], spread).astype(BF)

    def x_multiply(xr):
        for copy in load_w(ROUNDS + xr, xr):
            copy.wait()
        for copy in load_w(ROUNDS + 1 if xr == 0 else 2, 1 - xr):
            copy.start()
        for k in range(2):
            for part in range(2):
                rows = part * 512
                o = dot(hid[rows:rows + 512, :], wbuf[xr, k])
                pieces = []
                for outer in range(RING):
                    for inner in range(RING):
                        yy, zz = (inner, outer) if k == 0 else (outer, inner)
                        for b in range(4):
                            at = b * 128 + yy * 32 + zz * 8
                            pieces.append(o[at:at + 8])
                o = jnp.concatenate(pieces, axis=0).astype(BF)
                xbuf[k, xr, :, :, part * 32:(part + 1) * 32, :] = o.reshape(RING, RING, 32, WIDE)
            for hop in (2, 1, 3):
                to, dev = along(k, hop)
                remote(xbuf.at[k, xr, to], xr1.at[k, xr, mine[k]], xs1.at[k, xr], xq1.at[k, xr], n, dev)
            xr1[k, xr, mine[k]] = xbuf[k, xr, mine[k]]

    def x_forward(xr):
        for k in range(2):
            take(xr1.at[k, xr, pl.ds(0, RING - 1)], xq1.at[k, xr])
            own = mine[1 - k]
            for hop in (2, 1, 3):
                to, dev = along(1 - k, hop)
                remote(xr1.at[k, xr, :, to], xr2.at[k, xr, own], xs2.at[k, xr], xq2.at[k, xr], n, dev)
            xr2[k, xr, own] = xr1[k, xr, :, own]

    def x_combine(xr):
        for k in range(2):
            take(xr2.at[k, xr, pl.ds(0, RING - 1)], xq2.at[k, xr])
            part = dot(abig[k], xr2[k, xr].reshape(1024, WIDE))
            xpart[k, xr] = part.astype(BF).reshape(NODES, PACK, WIDE)
            for offset in NODE_OFFSETS:
                to = node_at(offset)
                remote(xpart.at[k, xr, to], xr3.at[k, xr, n], xs3.at[k, xr], xq3.at[k, xr], to, d)
            xr3[k, xr, n] = xpart[k, xr, n]
            weights = wg[k, :, :, (ROUNDS + xr) * WIDE:(ROUNDS + xr + 1) * WIDE].reshape(KS, WIDE)
            send_part(k, ROUNDS + xr, 0, WIDE, ROUNDS + 1 + xr, dot(hrecv[k].reshape(RING * TOK, KS), weights))

    def x_finish(xr):
        for k in range(2):
            take(xr3.at[k, xr, pl.ds(0, NODES - 1)], xq3.at[k, xr])
            routed = dot(place_back[...], xr3[k, xr].reshape(NODES * PACK, WIDE))
            finish(k, ROUNDS + xr, 0, WIDE, ROUNDS + 1 + xr, routed)


    def multiply(step):
        first = isinstance(step, int)
        slot = step % 2
        place = step % SLOTS
        for copy in load_w(step, slot):
            copy.wait()
        if first:
            for copy in load_w(1 if step == 0 else ROUNDS, 1 - slot):
                copy.start()
        else:
            @pl.when(step + 1 < ROUNDS)
            def _():
                for copy in load_w(step + 1, (step + 1) % 2):
                    copy.start()

            @pl.when(step >= SLOTS)
            def _():
                for k in range(2):
                    take(obuf.at[place, k, pl.ds(0, NODES - 1)], send1.at[place, k, 0])

        def send(k, lane, width, h):
            cols = pl.ds(lane, width)
            for offset in NODE_OFFSETS:
                to = node_at(offset)
                remote(
                    obuf.at[place, k, to, :, cols], recv1.at[k, step, n, :, cols],
                    send1.at[place, k, h], rsem1.at[k, step + h], to, d,
                )

        for k in range(2):
            for part in range(2):
                rows = part * 512
                o = dot(hid[rows:rows + 512, :], wbuf[slot, k])
                if k == 0:
                    o = jnp.concatenate(
                        [
                            o[b * 128 + yy * 32 + zz * 8:b * 128 + yy * 32 + zz * 8 + 8]
                            for b in range(4) for zz in range(RING) for yy in range(RING)
                        ],
                        axis=0,
                    )
                obuf[place, k, pl.ds(part * 4, 4)] = o.astype(BF).reshape(4, 128, WIDE)
            if first:
                send(k, 0, WIDE, 0)
            else:
                @pl.when(step < LAST)
                def _():
                    send(k, 0, WIDE, 0)

                @pl.when(step == LAST)
                def _():
                    for h in range(PARTS):
                        send(k, h * C, C, h)
            recv1[k, step, n] = obuf[place, k, n]

    def forward(k, step, lane, width, sem):
        cols = pl.ds(lane, width)
        take(recv1.at[k, step, pl.ds(0, NODES - 1), :, cols], rsem1.at[k, sem])
        for hop in (2, 1, 3):
            to, dev = along(k, hop)
            rows = pl.multiple_of(to * 32, 32)
            remote(
                recv1.at[k, step, :, pl.ds(rows, 32), cols], recv2.at[k, step, mine[k], :, :, cols],
                send2.at[k, sem], rsem2.at[k, sem], n, dev,
            )
        rows = pl.multiple_of(mine[k] * 32, 32)
        recv2[k, step, mine[k], :, :, cols] = recv1[k, step, :, pl.ds(rows, 32), cols]

    def combine(k, step, lane, width, sem):
        cols = pl.ds(lane, width)
        take(recv2.at[k, step, pl.ds(0, RING - 1), :, :, cols], rsem2.at[k, sem])
        slots = recv2[k, step, :, :, :, cols].reshape(1024, width)
        wide = pl.ds(pl.multiple_of(step * WIDE + lane, 128), width)
        weights = wg[k, :, :, wide].reshape(KS, width)
        send_part(k, step, lane, width, sem, dot(gbig[k], slots) + dot(hrecv[k].reshape(RING * TOK, KS), weights))

    def send_part(k, step, lane, width, sem, part):
        cols = pl.ds(lane, width)
        pbuf[k, step, :, :, cols] = part.astype(BF).reshape(RING, TOK, width)
        own = mine[1 - k]
        for hop in (2, 1, 3):
            to, dev = along(1 - k, hop)
            remote(
                pbuf.at[k, step, to, :, cols], recv3.at[k, step, own, :, cols],
                send3.at[k, sem], rsem3.at[k, sem], n, dev,
            )
        recv3[k, step, own, :, cols] = pbuf[k, step, own, :, cols]

    def finish(k, step, lane, width, sem, extra=None):
        cols = pl.ds(lane, width)
        take(recv3.at[k, step, pl.ds(0, RING - 1), :, cols], rsem3.at[k, sem])
        total = recv3[k, step, 0, :, cols].astype(F32)
        for j in range(1, RING):
            total += recv3[k, step, j, :, cols].astype(F32)
        if extra is not None:
            total += extra
        out_ref[:, pl.ds(pl.multiple_of(k * HALF + step * WIDE + lane, 128), width)] = total.astype(BF)

    def bulk(i, lag, act):
        @pl.when((i >= lag) & (i < LAST + lag))
        def _():
            for k in range(2):
                act(k, i - lag, 0, WIDE, i - lag)

    def last(i, lag, act):
        @pl.when(i == LAST + lag)
        def _():
            for k in range(2):
                for h in range(PARTS):
                    act(k, LAST, h * C, C, LAST + h)

    def loop(i, carry):
        @pl.when(i < ROUNDS)
        def _():
            multiply(i)

        bulk(i, AHEAD, forward)
        last(i, AHEAD, forward)

        @pl.when((i == 2) | (i == 3))
        def _():
            x_forward(i - 2)

        pl.when(i == AHEAD)(share_rows)
        pl.when(i == AHEAD + 2)(widen_gates)
        bulk(i, AHEAD + 2, combine)
        last(i, AHEAD + 1, combine)
        pl.when(i == AHEAD + 3)(widen_x)

        for xr in range(XR):
            @pl.when(i == AHEAD + 3 + xr)
            def _():
                x_combine(xr)

            @pl.when(i == AHEAD + 6 + xr)
            def _():
                x_finish(xr)

        bulk(i, AHEAD + 3, finish)
        last(i, AHEAD + 2, finish)
        return carry

    send_rows()
    hid_copy.wait()
    multiply(0)
    multiply(1)
    for xr in range(XR):
        x_multiply(xr)
    set_up()
    gate_pieces()
    lax.fori_loop(2, ROUNDS + AHEAD + 2, loop, 0)

    for k in range(2):
        take(hsend.at[k, pl.ds(0, RING - 1)], init_send.at[k])
        take(wg.at[k, pl.ds(0, RING - 1), :, pl.ds(0, QUART)], init_send.at[2 + k])
        take(wg.at[k, :, :, pl.ds(0, QUART)], init_send.at[6 + k])
        take(gsend.at[k, pl.ds(0, RING - 1)], init_send.at[4 + k])
        for xr in range(XR):
            take(xbuf.at[k, xr, pl.ds(0, RING - 1)], xs1.at[k, xr])
            take(xr2.at[k, xr, pl.ds(0, RING - 1)], xs2.at[k, xr])
            take(xpart.at[k, xr, pl.ds(0, NODES - 1)], xs3.at[k, xr])
        for step in range(ROUNDS - SLOTS, LAST):
            take(obuf.at[step % SLOTS, k, pl.ds(0, NODES - 1)], send1.at[step % SLOTS, k, 0])
        for h in range(PARTS):
            cols = pl.ds(h * C, C)
            take(obuf.at[LAST % SLOTS, k, pl.ds(0, NODES - 1), :, cols], send1.at[LAST % SLOTS, k, h])
            take(recv2.at[k, LAST, pl.ds(0, RING - 1), :, :, cols], send2.at[k, LAST + h])
            take(recv3.at[k, LAST, pl.ds(0, RING - 1), :, cols], send3.at[k, LAST + h])
        for xr in range(XR):
            take(recv3.at[k, ROUNDS + xr, pl.ds(0, RING - 1)], send3.at[k, ROUNDS + 1 + xr])
    take(asend.at[pl.ds(0, NODES - 1)], ash)

    def drain(step, carry):
        for k in range(2):
            take(recv2.at[k, step, pl.ds(0, RING - 1)], send2.at[k, step])
            take(recv3.at[k, step, pl.ds(0, RING - 1)], send3.at[k, step])
        return carry

    lax.fori_loop(0, LAST, drain, 0)


def body(expert_hidden, expert_down, shared_hidden, shared_down, expert_ids, gates):
    anywhere = pl.BlockSpec(memory_space=pl.ANY)
    vmem = pl.BlockSpec(memory_space=pltpu.VMEM)
    dma = pltpu.SemaphoreType.DMA
    return pl.pallas_call(
        kernel,
        out_shape=pltpu.VMEM((TOK, D), BF),
        in_specs=[anywhere] * 6,
        out_specs=vmem,
        scratch_shapes=[
            pltpu.VMEM((1024, EF), BF),
            pltpu.VMEM((TOK, EF), BF),
            pltpu.VMEM((TOP, TOK), jnp.int32),
            pltpu.VMEM((TOP, TOK), F32),
            pltpu.VMEM((2, 2, EF, WIDE), BF),
            pltpu.VMEM((SLOTS, 2, NODES, 128, WIDE), BF),
            pltpu.VMEM((2, ROUNDS, NODES, 128, WIDE), BF),
            pltpu.VMEM((2, ROUNDS, RING, NODES, 32, WIDE), BF),
            pltpu.VMEM((2, ALL, RING, TOK, WIDE), BF),
            pltpu.VMEM((2, ALL, RING, TOK, WIDE), BF),
            pltpu.VMEM((2, RING, 96, HALF), BF),
            pltpu.VMEM((2, RING * TOK, 1024), BF),
            pltpu.VMEM((2, RING, TOK, KS), BF),
            pltpu.VMEM((2, RING, TOK, 256), BF),
            pltpu.VMEM((2, RING, TOK, KS), BF),
            pltpu.VMEM((2, RING, TOK, 256), BF),
            pltpu.VMEM((2, XR, RING, RING, 64, WIDE), BF),
            pltpu.VMEM((2, XR, RING, RING, 64, WIDE), BF),
            pltpu.VMEM((2, XR, RING, RING, 64, WIDE), BF),
            pltpu.VMEM((2, XR, NODES, PACK, WIDE), BF),
            pltpu.VMEM((2, XR, NODES, PACK, WIDE), BF),
            pltpu.VMEM((2, NODES * PACK, 1024), BF),
            pltpu.VMEM((NODES, PACK, EXPERTS), BF),
            pltpu.VMEM((NODES, PACK, EXPERTS), BF),
            pltpu.VMEM((TOK, NODES * PACK), BF),
            dma,
            dma((2, 2)),
            dma((5,)),
            dma((8,)),
            dma((8,)),
            dma((SLOTS, 2, PARTS)),
            dma((2, ALL + 1)),
            dma((2, ALL + 1)),
            dma((2, ALL + 1)),
            dma((2, ALL + 1)),
            dma((2, ALL + 1)),
            dma((2, XR)),
            dma((2, XR)),
            dma((2, XR)),
            dma((2, XR)),
            dma((2, XR)),
            dma((2, XR)),
            dma,
            dma,
        ],
        compiler_params=pltpu.CompilerParams(
            collective_id=0, has_side_effects=True, vmem_limit_bytes=60 * 1024 * 1024
        ),
        name="combine",
    )(
        expert_hidden,
        expert_down.reshape(EF, D),
        shared_hidden,
        shared_down,
        expert_ids.T,
        gates.T,
    )


def solution(mesh):
    in_specs = (
        P(("node", "dev"), None),
        P(("node", "dev"), None, None),
        P(("node", "dev"), None),
        P("dev", None),
        P(("node", "dev"), None),
        P(("node", "dev"), None),
    )
    out_specs = P(("node", "dev"), None)
    return jax.shard_map(body, mesh=mesh, in_specs=in_specs, out_specs=out_specs, check_vma=False)
```
